128 devices in a mesh: src: 8 (over x_lo, z), tgt: 16 (over y, x_hi, core).
Axes of the slice: x: 4 (x_hi: 2, x_lo: 2; x = x_hi * 2 + x_lo), y: 4, z: 4, core: 2. Of those that a mesh axis runs over, the one named last changes fastest.
Arguments:
- coeff: float32 [1024, 640, 256], P(('src', 'tgt')), may hold values from -6 to 6
- factors: float32 [3, 1024, 512, 256], P(None, ('src', 'tgt')), may hold values from -0.25 to 0.25
Outputs:
- result: float32 [1024, 640, 256], P('src', 'tgt')
The draws below stay inside these ranges and needn't reach their ends.
All inputs are finite; a program needn't handle non-finite values.
Results may differ from the reference program's by a relative error of at most 0.0001.
Values sent between devices are 32-bit elements; how exact they have to be, the bound alone decides.
A program may use at most 128 MiB of HBM per device.

```python
import jax
import jax.numpy as jnp
from jax import lax

RANK = 256
BLK_DEV = 8
RHS = 640
LEVELS = 3
BLOCKS = 1024
N_SRC = 8
N_TGT = 16


def levels(stream_key, shape, pieces, smallest, top_value):
    def one(axis_at, parts):
        steps = jax.random.uniform(jax.random.fold_in(jax.random.fold_in(stream_key, 6), axis_at), (parts,), jnp.float32, smallest / len(pieces), top_value / len(pieces))
        return jnp.repeat(jnp.exp(steps), shape[axis_at] // parts).reshape((-1,) + (1,) * (len(shape) - axis_at - 1))

    loudness = one(*pieces[0])
    for cut in pieces[1:]:
        loudness = loudness * one(*cut)
    return loudness


def scatter_about(key, shape, deviation, limit, split=(), kind=jnp.bfloat16):
    array = jax.random.normal(key, shape, jnp.float32) * deviation
    if len(split) > 0:
        array = levels(key, shape, split, -0.22, 0.18) * array
    return jnp.clip(array, min=-limit, max=limit).astype(kind)


def setup_inputs(seed: int = 0) -> dict:
    streams_of = jax.random.split(jax.random.key(seed), 3)
    return {
        "coeff": scatter_about(streams_of[0], (BLOCKS, RHS, RANK), 1.0, 6.0, ((0, 128),), jnp.float32),
        "factors": scatter_about(streams_of[1], (LEVELS, BLOCKS, 2 * RANK, RANK), (2 * RANK) ** -0.5, 0.25, ((1, 128),), jnp.float32),
    }


def apply_level(coeff, factor, stride):
    count = coeff.shape[0]
    grouped = coeff.reshape(count // (2 * stride), 2, stride, RHS, RANK)
    lower = grouped[:, 0]
    higher = grouped[:, 1]
    tables = factor.reshape(count // (2 * stride), 2, stride, 2 * RANK, RANK)
    first = jnp.einsum("gmbr,gomrk->gombk", lower, tables[:, :, :, :RANK, :], precision=lax.Precision.HIGHEST)
    second = jnp.einsum("gmbr,gomrk->gombk", higher, tables[:, :, :, RANK:, :], precision=lax.Precision.HIGHEST)
    return (first + second).reshape(count, RHS, RANK)


def reference(coeff, factors):
    strides = [BLK_DEV * N_TGT // 2, BLK_DEV * N_TGT * N_SRC // 2, BLK_DEV]
    state = coeff
    for level in range(LEVELS):
        state = apply_level(state, factors[level], strides[level])
    return state
```

```python
import functools

import jax
import jax.numpy as jnp
from jax import lax
from jax.experimental import pallas as pl
from jax.experimental.pallas import tpu as pltpu
from jax.sharding import PartitionSpec as P

SPLIT = 4
AHEAD = 6
HOLD = 29
STEP = 0
MESH = pl.DeviceIdType.MESH


def split(x):
    high = x.astype(jnp.bfloat16)
    return high, (x - high.astype(jnp.float32)).astype(jnp.bfloat16)


def dot(x, w):
    x_high, x_low = split(x)
    w_high, w_low = split(w)
    mm = functools.partial(jnp.dot, preferred_element_type=jnp.float32)
    return mm(x_high, w_high) + (mm(x_high, w_low) + mm(x_low, w_high))


def kernel(
    n_src, n_tgt, coeff, factors, out,
    c_v, f_v, got0, got1, got2, new0, new1, new2,
    c_sem, f_sem, got0_sem, got1_sem, got2_sem, sent0, sent1, sent2, sent3, landed,
):
    blocks, rhs, rank = c_v.shape
    rows = rhs // SPLIT
    part = rhs // n_tgt
    count = blocks * SPLIT
    src = lax.axis_index("src")
    tgt = lax.axis_index("tgt")
    half_t, half_s = n_tgt // 2, n_src // 2
    upper = (tgt // half_t, src // half_s, lax.rem(tgt, 2))
    first = (src, lax.rem(tgt + half_t, n_tgt))
    second = (lax.rem(src + half_s, n_src), tgt)
    third = (src, tgt + 1 - 2 * lax.rem(tgt, 2))

    def load_c(block):
        return pltpu.make_async_copy(coeff.at[block], c_v.at[block], c_sem.at[block])

    def load_f(level, block):
        return pltpu.make_async_copy(
            factors.at[level, block], f_v.at[level, block], f_sem.at[level, block]
        )

    def place(chunk):
        block = chunk // SPLIT
        at = pl.multiple_of(lax.rem(chunk, SPLIT) * rows, rows)
        return block, pl.ds(at, rows)

    def exchange(source, target, sent, got, device, chunk):
        block, span = place(chunk)
        return pltpu.make_async_remote_copy(
            source.at[block, span, :], target.at[block, span, :], sent, got.at[chunk],
            device_id=device, device_id_type=MESH,
        )

    def exchange0(chunk):
        return exchange(coeff, got0, sent0, got0_sem, first, chunk)

    def exchange1(chunk):
        return exchange(new0, got1, sent1, got1_sem, second, chunk)

    def exchange2(chunk):
        return exchange(new1, got2, sent2, got2_sem, third, chunk)

    def combine(level, chunk, own, other, target):
        block, span = place(chunk)
        own_rows = pl.ds(pl.multiple_of(upper[level] * rank, rank), rank)
        other_rows = pl.ds(pl.multiple_of((1 - upper[level]) * rank, rank), rank)
        target[block, span, :] = dot(own[block, span, :], f_v[level, block, own_rows, :]) + dot(
            other[block, span, :], f_v[level, block, other_rows, :]
        )

    def scatter(block):
        out[tgt * blocks + block] = new2[block, pl.ds(pl.multiple_of(tgt * part, 8), part), :]

        @pl.loop(1, n_tgt)
        def _(k):
            to = lax.rem(tgt + k, n_tgt)
            pltpu.make_async_remote_copy(
                new2.at[block, pl.ds(pl.multiple_of(to * part, 8), part), :],
                out.at[tgt * blocks + block], sent3, landed,
                device_id=(src, to), device_id_type=MESH,
            ).start()

    @pl.loop(0, blocks)
    def _(block):
        load_c(block).start()
        load_f(0, block).start()

    barrier = pltpu.get_barrier_semaphore()

    @pl.loop(1, n_tgt)
    def _(k):
        pl.semaphore_signal(
            barrier, inc=1, device_id=(src, lax.rem(tgt + k, n_tgt)), device_id_type=MESH
        )

    pl.semaphore_signal(barrier, inc=1, device_id=second, device_id_type=MESH)
    pl.semaphore_wait(barrier, n_tgt)

    @pl.loop(0, AHEAD)
    def _(chunk):
        exchange0(chunk).start()

    @pl.loop(0, blocks)
    def _(block):
        load_f(1, block).start()
        load_f(2, block).start()

    @pl.loop(0, count + 2)
    def _(step):
        @pl.when(step + AHEAD < count)
        def _():
            exchange0(step + AHEAD).start()

        @pl.when(step < count)
        def _():
            block = step // SPLIT

            @pl.when(lax.rem(step, SPLIT) == 0)
            def _():
                load_c(block).wait()
                load_f(0, block).wait()

            exchange0(step).wait_recv()
            combine(0, step, c_v, got0, new0)
            exchange1(step).start()

        @pl.when((step >= 1) & (step < count + 1))
        def _():
            chunk = step - 1

            @pl.when(lax.rem(chunk, SPLIT) == 0)
            def _():
                load_f(1, chunk // SPLIT).wait()

            exchange1(chunk).wait_recv()
            combine(1, chunk, new0, got1, new1)
            exchange2(chunk).start()

        @pl.when(step >= 2)
        def _():
            chunk = step - 2

            @pl.when(lax.rem(chunk, SPLIT) == 0)
            def _():
                load_f(2, chunk // SPLIT).wait()

            exchange2(chunk).wait_recv()
            combine(2, chunk, new1, got2, new2)

        for block in range(blocks):
            ready = (block + 1) * SPLIT + 1

            @pl.when(step == max(ready, HOLD + STEP * block))
            def _(block=block):
                scatter(block)

    for copy in (
        pltpu.make_async_remote_copy(coeff, got0, sent0, landed, device_id=first, device_id_type=MESH),
        pltpu.make_async_remote_copy(new0, got1, sent1, landed, device_id=second, device_id_type=MESH),
        pltpu.make_async_remote_copy(new1, got2, sent2, landed, device_id=third, device_id_type=MESH),
    ):
        copy.wait_send()
    moved = out.at[pl.ds(0, (n_tgt - 1) * blocks)]
    last = pltpu.make_async_remote_copy(
        moved, moved, sent3, landed, device_id=third, device_id_type=MESH
    )
    last.wait_send()
    last.wait_recv()


def solution(mesh):
    n_src, n_tgt = mesh.shape["src"], mesh.shape["tgt"]

    def local(coeff, factors):
        blocks, rhs, rank = coeff.shape
        levels = factors.shape[0]
        count = blocks * SPLIT
        whole = pltpu.VMEM((blocks, rhs, rank), jnp.float32)
        dma = pltpu.SemaphoreType.DMA
        return pl.pallas_call(
            functools.partial(kernel, n_src, n_tgt),
            out_shape=jax.ShapeDtypeStruct((n_tgt * blocks, rhs // n_tgt, rank), jnp.float32),
            in_specs=[pl.BlockSpec(memory_space=pl.ANY)] * 2,
            out_specs=pl.BlockSpec(memory_space=pltpu.VMEM),
            scratch_shapes=[
                whole, pltpu.VMEM(factors.shape, jnp.float32), whole, whole, whole, whole, whole, whole,
                dma((blocks,)), dma((levels, blocks)), dma((count,)), dma((count,)), dma((count,)),
                dma, dma, dma, dma, dma,
            ],
            compiler_params=pltpu.CompilerParams(
                collective_id=0, has_side_effects=True, vmem_limit_bytes=60 * 1024 * 1024
            ),
        )(coeff, factors)

    placed = (P(("src", "tgt"), None, None), P(None, ("src", "tgt"), None, None))
    return jax.shard_map(
        local, mesh=mesh, in_specs=placed, out_specs=P("src", "tgt", None), check_vma=False
    )
```

```python
import functools

import jax
import jax.numpy as jnp
from jax import lax
from jax.experimental import pallas as pl
from jax.experimental.pallas import tpu as pltpu
from jax.sharding import PartitionSpec as P

SPLIT = 8
AHEAD = 24
LAG_B, LAG_C = 3, 5
HOLD_Y, STEP_Y = 58, 1
HOLD_XY, STEP_XY = 64, 0
ORDER = (1, 3, 2)
MESH = pl.DeviceIdType.MESH


def split(x):
    high = x.astype(jnp.bfloat16)
    return high, (x - high.astype(jnp.float32)).astype(jnp.bfloat16)


def dot(x, w):
    x_high, x_low = split(x)
    w_high, w_low = split(w)
    mm = functools.partial(jnp.dot, preferred_element_type=jnp.float32)
    return mm(x_high, w_high) + (mm(x_high, w_low) + mm(x_low, w_high))


def kernel(
    n_src, n_tgt, coeff, factors, out,
    c_v, f_v, got0, got1, got2, new0, new1, new2,
    c_sem, f_sem, got0_sem, got1_sem, got2_sem, sent0, sent1, sent2, sent3, landed,
):
    blocks, rhs, rank = c_v.shape
    rows = rhs // SPLIT
    part = rhs // n_tgt
    count = blocks * SPLIT
    src = lax.axis_index("src")
    tgt = lax.axis_index("tgt")
    half_t, half_s = n_tgt // 2, n_src // 2
    upper = (tgt // half_t, src // half_s, lax.rem(tgt, 2))
    first = (src, lax.rem(tgt + half_t, n_tgt))
    second = (lax.rem(src + half_s, n_src), tgt)
    third = (src, tgt + 1 - 2 * lax.rem(tgt, 2))

    def load_c(block):
        return pltpu.make_async_copy(coeff.at[block], c_v.at[block], c_sem.at[block])

    def load_f(level, block):
        return pltpu.make_async_copy(
            factors.at[level, block], f_v.at[level, block], f_sem.at[level, block]
        )

    def place(chunk):
        block = chunk // SPLIT
        at = pl.multiple_of(lax.rem(chunk, SPLIT) * rows, rows)
        return block, pl.ds(at, rows)

    def exchange(source, target, sent, got, device, chunk):
        block, span = place(chunk)
        return pltpu.make_async_remote_copy(
            source.at[block, span, :], target.at[block, span, :], sent, got.at[chunk],
            device_id=device, device_id_type=MESH,
        )

    def exchange0(chunk):
        return exchange(c_v, got0, sent0, got0_sem, first, chunk)

    def exchange1(chunk):
        return exchange(new0, got1, sent1, got1_sem, second, chunk)

    def exchange2(chunk):
        return exchange(new1, got2, sent2, got2_sem, third, chunk)

    def send0(chunk):
        @pl.when(lax.rem(chunk, SPLIT) == 0)
        def _():
            load_c(chunk // SPLIT).wait()

        exchange0(chunk).start()

    def combine(level, chunk, own, other, target):
        block, span = place(chunk)
        own_rows = pl.ds(pl.multiple_of(upper[level] * rank, rank), rank)
        other_rows = pl.ds(pl.multiple_of((1 - upper[level]) * rank, rank), rank)
        target[block, span, :] = dot(own[block, span, :], f_v[level, block, own_rows, :]) + dot(
            other[block, span, :], f_v[level, block, other_rows, :]
        )

    y, x, core = tgt // 4, lax.rem(tgt // 2, 2), lax.rem(tgt, 2)

    def deliver(block, dy, other_x, other_core):
        to_x = 1 - x if other_x else x
        to_core = 1 - core if other_core else core
        to = lax.rem(y + dy, n_tgt // 4) * 4 + to_x * 2 + to_core
        pltpu.make_async_remote_copy(
            new2.at[block, pl.ds(pl.multiple_of(to * part, 8), part), :],
            out.at[tgt * blocks + block], sent3, landed,
            device_id=(src, to), device_id_type=MESH,
        ).start()

    def scatter_x(block):
        out[tgt * blocks + block] = new2[block, pl.ds(pl.multiple_of(tgt * part, 8), part), :]
        for other in (0, 1):
            deliver(block, 0, 1, other)

    def scatter_y(block):
        for dy in ORDER:
            for other in (0, 1):
                deliver(block, dy, 0, other)
        deliver(block, 0, 0, 1)

    def scatter_xy(block):
        for dy in ORDER:
            for other in (0, 1):
                deliver(block, dy, 1, other)

    barrier = pltpu.get_barrier_semaphore()

    @pl.loop(1, n_tgt)
    def _(k):
        pl.semaphore_signal(
            barrier, inc=1, device_id=(src, lax.rem(tgt + k, n_tgt)), device_id_type=MESH
        )

    pl.semaphore_signal(barrier, inc=1, device_id=second, device_id_type=MESH)
    load_c(0).start()
    load_f(0, 0).start()

    @pl.loop(1, blocks)
    def _(block):
        load_c(block).start()
        load_f(0, block).start()

    pl.semaphore_wait(barrier, n_tgt)

    @pl.loop(0, AHEAD)
    def _(chunk):
        send0(chunk)

    @pl.loop(0, blocks)
    def _(block):
        load_f(1, block).start()
        load_f(2, block).start()

    @pl.loop(0, count + LAG_C)
    def _(step):
        @pl.when(step + AHEAD < count)
        def _():
            send0(step + AHEAD)

        @pl.when(step < count)
        def _():
            block = step // SPLIT

            @pl.when(lax.rem(step, SPLIT) == 0)
            def _():
                load_f(0, block).wait()

            exchange0(step).wait_recv()
            combine(0, step, c_v, got0, new0)
            exchange1(step).start()

        @pl.when((step >= LAG_B) & (step < count + LAG_B))
        def _():
            chunk = step - LAG_B

            @pl.when(lax.rem(chunk, SPLIT) == 0)
            def _():
                load_f(1, chunk // SPLIT).wait()

            exchange1(chunk).wait_recv()
            combine(1, chunk, new0, got1, new1)
            exchange2(chunk).start()

        @pl.when(step >= LAG_C)
        def _():
            chunk = step - LAG_C

            @pl.when(lax.rem(chunk, SPLIT) == 0)
            def _():
                load_f(2, chunk // SPLIT).wait()

            exchange2(chunk).wait_recv()
            combine(2, chunk, new1, got2, new2)

        for block in range(blocks):
            ready = (block + 1) * SPLIT - 1 + LAG_C

            @pl.when(step == max(ready, HOLD_Y + STEP_Y * min(block, blocks - 2)))
            def _(block=block):
                scatter_y(block)

            @pl.when(step == max(ready, HOLD_XY + STEP_XY * min(block, blocks - 2)))
            def _(block=block):
                scatter_xy(block)

    @pl.loop(0, blocks)
    def _(block):
        scatter_x(block)

    for copy in (
        pltpu.make_async_remote_copy(c_v, got0, sent0, landed, device_id=first, device_id_type=MESH),
        pltpu.make_async_remote_copy(new0, got1, sent1, landed, device_id=second, device_id_type=MESH),
        pltpu.make_async_remote_copy(new1, got2, sent2, landed, device_id=third, device_id_type=MESH),
    ):
        copy.wait_send()
    moved = out.at[pl.ds(0, (n_tgt - 1) * blocks)]
    last = pltpu.make_async_remote_copy(
        moved, moved, sent3, landed, device_id=third, device_id_type=MESH
    )
    last.wait_send()
    last.wait_recv()


def store(source, out, sem):
    pieces = 8
    size = source.shape[0] // pieces
    copies = [
        pltpu.make_async_copy(source.at[pl.ds(i * size, size)], out.at[pl.ds(i * size, size)], sem.at[i])
        for i in range(pieces)
    ]
    for copy in copies:
        copy.start()
    for copy in copies:
        copy.wait()


def solution(mesh):
    n_src, n_tgt = mesh.shape["src"], mesh.shape["tgt"]

    def local(coeff, factors):
        blocks, rhs, rank = coeff.shape
        levels = factors.shape[0]
        count = blocks * SPLIT
        whole = pltpu.VMEM((blocks, rhs, rank), jnp.float32)
        dma = pltpu.SemaphoreType.DMA
        shape = (n_tgt * blocks, rhs // n_tgt, rank)
        landed = pl.pallas_call(
            functools.partial(kernel, n_src, n_tgt),
            out_shape=pltpu.VMEM(shape, jnp.float32),
            in_specs=[pl.BlockSpec(memory_space=pl.ANY)] * 2,
            out_specs=pl.BlockSpec(memory_space=pltpu.VMEM),
            scratch_shapes=[
                whole, pltpu.VMEM(factors.shape, jnp.float32), whole, whole, whole, whole, whole, whole,
                dma((blocks,)), dma((levels, blocks)), dma((count,)), dma((count,)), dma((count,)),
                dma, dma, dma, dma, dma,
            ],
            compiler_params=pltpu.CompilerParams(
                collective_id=0, has_side_effects=True, vmem_limit_bytes=54 * 1024 * 1024
            ),
        )(coeff, factors)
        return landed

    placed = (P(("src", "tgt"), None, None), P(None, ("src", "tgt"), None, None))
    return jax.shard_map(
        local, mesh=mesh, in_specs=placed, out_specs=P("src", "tgt", None), check_vma=False
    )
```

```python
import functools

import jax
import jax.numpy as jnp
from jax import lax
from jax.experimental import pallas as pl
from jax.experimental.pallas import tpu as pltpu
from jax.sharding import PartitionSpec as P

SPLIT = 8
AHEAD = 24
LAG_B, LAG_C = 3, 5
HOLD_Y, STEP_Y = 58, 1
HOLD_XY, STEP_XY = 64, 0
ORDER = (1, 3, 2)
MESH = pl.DeviceIdType.MESH


def split(x):
    high = x.astype(jnp.bfloat16)
    return high, (x - high.astype(jnp.float32)).astype(jnp.bfloat16)


def dot(x, w):
    x_high, x_low = split(x)
    w_high, w_low = split(w)
    mm = functools.partial(jnp.dot, preferred_element_type=jnp.float32)
    return mm(x_high, w_high) + (mm(x_high, w_low) + mm(x_low, w_high))


def kernel(
    n_src, n_tgt, coeff, factors, out,
    c_v, f_v, got0, got1, got2, new0, new1, new2,
    c_sem, f_sem, got0_sem, got1_sem, got2_sem, sent0, sent1, sent2, sent3, landed, near, far,
):
    blocks, rhs, rank = c_v.shape
    rows = rhs // SPLIT
    part = rhs // n_tgt
    count = blocks * SPLIT
    src = lax.axis_index("src")
    tgt = lax.axis_index("tgt")
    half_t, half_s = n_tgt // 2, n_src // 2
    upper = (tgt // half_t, src // half_s, lax.rem(tgt, 2))
    first = (src, lax.rem(tgt + half_t, n_tgt))
    second = (lax.rem(src + half_s, n_src), tgt)
    third = (src, tgt + 1 - 2 * lax.rem(tgt, 2))

    def load_c(block):
        return pltpu.make_async_copy(coeff.at[block], c_v.at[block], c_sem.at[block])

    def load_f(level, block):
        return pltpu.make_async_copy(
            factors.at[level, block], f_v.at[level, block], f_sem.at[level, block]
        )

    def place(chunk):
        block = chunk // SPLIT
        at = pl.multiple_of(lax.rem(chunk, SPLIT) * rows, rows)
        return block, pl.ds(at, rows)

    def exchange(source, target, sent, got, device, chunk):
        block, span = place(chunk)
        return pltpu.make_async_remote_copy(
            source.at[block, span, :], target.at[block, span, :], sent, got.at[chunk],
            device_id=device, device_id_type=MESH,
        )

    def exchange0(chunk):
        return exchange(c_v, got0, sent0, got0_sem, first, chunk)

    def exchange1(chunk):
        return exchange(new0, got1, sent1, got1_sem, second, chunk)

    def exchange2(chunk):
        return exchange(new1, got2, sent2, got2_sem, third, chunk)

    def send0(chunk):
        @pl.when(lax.rem(chunk, SPLIT) == 0)
        def _():
            load_c(chunk // SPLIT).wait()

        exchange0(chunk).start()

    def combine(level, chunk, own, other, target):
        block, span = place(chunk)
        own_rows = pl.ds(pl.multiple_of(upper[level] * rank, rank), rank)
        other_rows = pl.ds(pl.multiple_of((1 - upper[level]) * rank, rank), rank)
        target[block, span, :] = dot(own[block, span, :], f_v[level, block, own_rows, :]) + dot(
            other[block, span, :], f_v[level, block, other_rows, :]
        )

    y, x, core = tgt // 4, lax.rem(tgt // 2, 2), lax.rem(tgt, 2)

    def deliver(block, dy, other_x, other_core):
        to_x = 1 - x if other_x else x
        to_core = 1 - core if other_core else core
        to = lax.rem(y + dy, n_tgt // 4) * 4 + to_x * 2 + to_core
        pltpu.make_async_remote_copy(
            new2.at[block, pl.ds(pl.multiple_of(to * part, 8), part), :],
            out.at[tgt * blocks + block], sent3, landed,
            device_id=(src, to), device_id_type=MESH,
        ).start()

    def scatter_x(block):
        out[tgt * blocks + block] = new2[block, pl.ds(pl.multiple_of(tgt * part, 8), part), :]
        for other in (0, 1):
            deliver(block, 0, 1, other)

    def scatter_y(block):
        for dy in ORDER:
            for other in (0, 1):
                deliver(block, dy, 0, other)
        deliver(block, 0, 0, 1)

    def scatter_xy(block):
        for dy in ORDER:
            for other in (0, 1):
                deliver(block, dy, 1, other)

    barrier = pltpu.get_barrier_semaphore()

    def greet(semaphore, device):
        pl.semaphore_signal(semaphore, inc=1, device_id=device, device_id_type=MESH)

    beside = (src, tgt + 2 - 4 * x)
    for dy in (2, 1, 3):
        greet(barrier, (src, lax.rem(tgt + 4 * dy, n_tgt)))
    for device in (second, beside, third):
        greet(barrier, device)
    load_c(0).start()
    load_f(0, 0).start()

    @pl.loop(1, blocks)
    def _(block):
        load_c(block).start()
        load_f(0, block).start()

    pl.semaphore_wait(barrier, 6)
    greet(near, third)

    @pl.loop(0, AHEAD)
    def _(chunk):
        send0(chunk)

    @pl.loop(0, blocks)
    def _(block):
        load_f(1, block).start()
        load_f(2, block).start()

    pl.semaphore_wait(near, 1)
    greet(far, beside)
    pl.semaphore_wait(far, 1)

    @pl.loop(0, count + LAG_C)
    def _(step):
        @pl.when(step + AHEAD < count)
        def _():
            send0(step + AHEAD)

        @pl.when(step < count)
        def _():
            block = step // SPLIT

            @pl.when(lax.rem(step, SPLIT) == 0)
            def _():
                load_f(0, block).wait()

            exchange0(step).wait_recv()
            combine(0, step, c_v, got0, new0)
            exchange1(step).start()

        @pl.when((step >= LAG_B) & (step < count + LAG_B))
        def _():
            chunk = step - LAG_B

            @pl.when(lax.rem(chunk, SPLIT) == 0)
            def _():
                load_f(1, chunk // SPLIT).wait()

            exchange1(chunk).wait_recv()
            combine(1, chunk, new0, got1, new1)
            exchange2(chunk).start()

        @pl.when(step >= LAG_C)
        def _():
            chunk = step - LAG_C

            @pl.when(lax.rem(chunk, SPLIT) == 0)
            def _():
                load_f(2, chunk // SPLIT).wait()

            exchange2(chunk).wait_recv()
            combine(2, chunk, new1, got2, new2)

        for block in range(blocks):
            ready = (block + 1) * SPLIT - 1 + LAG_C

            @pl.when(step == max(ready, HOLD_Y + STEP_Y * min(block, blocks - 2)))
            def _(block=block):
                scatter_y(block)

            @pl.when(step == max(ready, HOLD_XY + STEP_XY * min(block, blocks - 2)))
            def _(block=block):
                scatter_xy(block)

    @pl.loop(0, blocks)
    def _(block):
        scatter_x(block)

    for copy in (
        pltpu.make_async_remote_copy(c_v, got0, sent0, landed, device_id=first, device_id_type=MESH),
        pltpu.make_async_remote_copy(new0, got1, sent1, landed, device_id=second, device_id_type=MESH),
        pltpu.make_async_remote_copy(new1, got2, sent2, landed, device_id=third, device_id_type=MESH),
    ):
        copy.wait_send()
    moved = out.at[pl.ds(0, (n_tgt - 1) * blocks)]
    last = pltpu.make_async_remote_copy(
        moved, moved, sent3, landed, device_id=third, device_id_type=MESH
    )
    last.wait_send()
    last.wait_recv()


def store(source, out, sem):
    pieces = 8
    size = source.shape[0] // pieces
    copies = [
        pltpu.make_async_copy(source.at[pl.ds(i * size, size)], out.at[pl.ds(i * size, size)], sem.at[i])
        for i in range(pieces)
    ]
    for copy in copies:
        copy.start()
    for copy in copies:
        copy.wait()


def solution(mesh):
    n_src, n_tgt = mesh.shape["src"], mesh.shape["tgt"]

    def local(coeff, factors):
        blocks, rhs, rank = coeff.shape
        levels = factors.shape[0]
        count = blocks * SPLIT
        whole = pltpu.VMEM((blocks, rhs, rank), jnp.float32)
        dma = pltpu.SemaphoreType.DMA
        shape = (n_tgt * blocks, rhs // n_tgt, rank)
        landed = pl.pallas_call(
            functools.partial(kernel, n_src, n_tgt),
            out_shape=pltpu.VMEM(shape, jnp.float32),
            in_specs=[pl.BlockSpec(memory_space=pl.ANY)] * 2,
            out_specs=pl.BlockSpec(memory_space=pltpu.VMEM),
            scratch_shapes=[
                whole, pltpu.VMEM(factors.shape, jnp.float32), whole, whole, whole, whole, whole, whole,
                dma((blocks,)), dma((levels, blocks)), dma((count,)), dma((count,)), dma((count,)),
                dma, dma, dma, dma, dma, pltpu.SemaphoreType.REGULAR, pltpu.SemaphoreType.REGULAR,
            ],
            compiler_params=pltpu.CompilerParams(
                collective_id=0, has_side_effects=True, vmem_limit_bytes=54 * 1024 * 1024
            ),
        )(coeff, factors)
        return landed

    placed = (P(("src", "tgt"), None, None), P(None, ("src", "tgt"), None, None))
    return jax.shard_map(
        local, mesh=mesh, in_specs=placed, out_specs=P("src", "tgt", None), check_vma=False
    )
```

```python
import functools

import jax
import jax.numpy as jnp
from jax import lax
from jax.experimental import pallas as pl
from jax.experimental.pallas import tpu as pltpu
from jax.sharding import PartitionSpec as P

SPLIT = 8
AHEAD = 24
FIRST = 3
LAG_B, LAG_C = 3, 5
HOLD_Y, STEP_Y = 58, 1
HOLD_XY, STEP_XY = 54, 2
ORDER = (1, 3, 2)
MESH = pl.DeviceIdType.MESH


def split(x):
    high = x.astype(jnp.bfloat16)
    return high, (x - high.astype(jnp.float32)).astype(jnp.bfloat16)


def dot(x, w):
    x_high, x_low = split(x)
    w_high, w_low = split(w)
    mm = functools.partial(jnp.dot, preferred_element_type=jnp.float32)
    return mm(x_high, w_high) + (mm(x_high, w_low) + mm(x_low, w_high))


def kernel(
    n_src, n_tgt, coeff, factors, out,
    c_v, f_v, got0, got1, got2, new0, new1, new2,
    c_sem, f_sem, got0_sem, got1_sem, got2_sem, sent0, sent1, sent2, sent3, landed, near, far,
):
    blocks, rhs, rank = c_v.shape
    rows = rhs // SPLIT
    part = rhs // n_tgt
    count = blocks * SPLIT
    src = lax.axis_index("src")
    tgt = lax.axis_index("tgt")
    half_t, half_s = n_tgt // 2, n_src // 2
    upper = (tgt // half_t, src // half_s, lax.rem(tgt, 2))
    first = (src, lax.rem(tgt + half_t, n_tgt))
    second = (lax.rem(src + half_s, n_src), tgt)
    third = (src, tgt + 1 - 2 * lax.rem(tgt, 2))

    def load_c(block):
        return pltpu.make_async_copy(coeff.at[block], c_v.at[block], c_sem.at[block])

    def load_f(level, block):
        return pltpu.make_async_copy(
            factors.at[level, block], f_v.at[level, block], f_sem.at[level, block]
        )

    def place(chunk):
        block = chunk // SPLIT
        at = pl.multiple_of(lax.rem(chunk, SPLIT) * rows, rows)
        return block, pl.ds(at, rows)

    def exchange(source, target, sent, got, device, chunk):
        block, span = place(chunk)
        return pltpu.make_async_remote_copy(
            source.at[block, span, :], target.at[block, span, :], sent, got.at[chunk],
            device_id=device, device_id_type=MESH,
        )

    def exchange0(chunk):
        return exchange(c_v, got0, sent0, got0_sem, first, chunk)

    def exchange1(chunk):
        return exchange(new0, got1, sent1, got1_sem, second, chunk)

    def exchange2(chunk):
        return exchange(new1, got2, sent2, got2_sem, third, chunk)

    def send0(chunk):
        @pl.when(lax.rem(chunk, SPLIT) == 0)
        def _():
            load_c(chunk // SPLIT).wait()

        exchange0(chunk).start()

    def combine(level, chunk, own, other, target):
        block, span = place(chunk)
        own_rows = pl.ds(pl.multiple_of(upper[level] * rank, rank), rank)
        other_rows = pl.ds(pl.multiple_of((1 - upper[level]) * rank, rank), rank)
        target[block, span, :] = dot(own[block, span, :], f_v[level, block, own_rows, :]) + dot(
            other[block, span, :], f_v[level, block, other_rows, :]
        )

    y, x, core = tgt // 4, lax.rem(tgt // 2, 2), lax.rem(tgt, 2)

    def deliver(block, dy, other_x, other_core):
        to_x = 1 - x if other_x else x
        to_core = 1 - core if other_core else core
        to = lax.rem(y + dy, n_tgt // 4) * 4 + to_x * 2 + to_core
        pltpu.make_async_remote_copy(
            new2.at[block, pl.ds(pl.multiple_of(to * part, 8), part), :],
            out.at[tgt * blocks + block], sent3, landed,
            device_id=(src, to), device_id_type=MESH,
        ).start()

    def scatter_x(block):
        out[tgt * blocks + block] = new2[block, pl.ds(pl.multiple_of(tgt * part, 8), part), :]
        for other in (0, 1):
            deliver(block, 0, 1, other)

    def scatter_y(block):
        for dy in ORDER:
            for other in (0, 1):
                deliver(block, dy, 0, other)
        deliver(block, 0, 0, 1)

    def scatter_xy(block):
        for dy in ORDER:
            for other in (0, 1):
                deliver(block, dy, 1, other)

    barrier = pltpu.get_barrier_semaphore()

    def greet(semaphore, device):
        pl.semaphore_signal(semaphore, inc=1, device_id=device, device_id_type=MESH)

    beside = (src, tgt + 2 - 4 * x)
    for dy in (2, 1, 3):
        greet(barrier, (src, lax.rem(tgt + 4 * dy, n_tgt)))
    for device in (second, beside, third):
        greet(barrier, device)
    for block in range(FIRST):
        load_c(block).start()
    load_f(0, 0).start()

    pl.semaphore_wait(barrier, 6)
    greet(near, third)

    @pl.loop(0, AHEAD)
    def _(chunk):
        send0(chunk)

    @pl.loop(1, blocks)
    def _(block):
        @pl.when(block >= FIRST)
        def _():
            load_c(block).start()

        load_f(0, block).start()

    @pl.loop(0, blocks)
    def _(block):
        load_f(1, block).start()
        load_f(2, block).start()

    pl.semaphore_wait(near, 1)
    greet(far, beside)
    pl.semaphore_wait(far, 1)

    @pl.loop(0, count + LAG_C)
    def _(step):
        @pl.when(step + AHEAD < count)
        def _():
            send0(step + AHEAD)

        @pl.when(step < count)
        def _():
            block = step // SPLIT

            @pl.when(lax.rem(step, SPLIT) == 0)
            def _():
                load_f(0, block).wait()

            exchange0(step).wait_recv()
            combine(0, step, c_v, got0, new0)
            exchange1(step).start()

        @pl.when((step >= LAG_B) & (step < count + LAG_B))
        def _():
            chunk = step - LAG_B

            @pl.when(lax.rem(chunk, SPLIT) == 0)
            def _():
                load_f(1, chunk // SPLIT).wait()

            exchange1(chunk).wait_recv()
            combine(1, chunk, new0, got1, new1)
            exchange2(chunk).start()

        @pl.when(step >= LAG_C)
        def _():
            chunk = step - LAG_C

            @pl.when(lax.rem(chunk, SPLIT) == 0)
            def _():
                load_f(2, chunk // SPLIT).wait()

            exchange2(chunk).wait_recv()
            combine(2, chunk, new1, got2, new2)

        for block in range(blocks):
            ready = (block + 1) * SPLIT - 1 + LAG_C

            @pl.when(step == max(ready, HOLD_Y + STEP_Y * min(block, blocks - 2)))
            def _(block=block):
                scatter_y(block)

            @pl.when(step == max(ready, HOLD_XY + STEP_XY * min(block, blocks - 2)))
            def _(block=block):
                scatter_xy(block)

    @pl.loop(0, blocks)
    def _(block):
        scatter_x(block)

    for copy in (
        pltpu.make_async_remote_copy(c_v, got0, sent0, landed, device_id=first, device_id_type=MESH),
        pltpu.make_async_remote_copy(new0, got1, sent1, landed, device_id=second, device_id_type=MESH),
        pltpu.make_async_remote_copy(new1, got2, sent2, landed, device_id=third, device_id_type=MESH),
    ):
        copy.wait_send()
    moved = out.at[pl.ds(0, (n_tgt - 1) * blocks)]
    last = pltpu.make_async_remote_copy(
        moved, moved, sent3, landed, device_id=third, device_id_type=MESH
    )
    last.wait_send()
    last.wait_recv()


def store(source, out, sem):
    pieces = 8
    size = source.shape[0] // pieces
    copies = [
        pltpu.make_async_copy(source.at[pl.ds(i * size, size)], out.at[pl.ds(i * size, size)], sem.at[i])
        for i in range(pieces)
    ]
    for copy in copies:
        copy.start()
    for copy in copies:
        copy.wait()


def solution(mesh):
    n_src, n_tgt = mesh.shape["src"], mesh.shape["tgt"]

    def local(coeff, factors):
        blocks, rhs, rank = coeff.shape
        levels = factors.shape[0]
        count = blocks * SPLIT
        whole = pltpu.VMEM((blocks, rhs, rank), jnp.float32)
        dma = pltpu.SemaphoreType.DMA
        shape = (n_tgt * blocks, rhs // n_tgt, rank)
        landed = pl.pallas_call(
            functools.partial(kernel, n_src, n_tgt),
            out_shape=pltpu.VMEM(shape, jnp.float32),
            in_specs=[pl.BlockSpec(memory_space=pl.ANY)] * 2,
            out_specs=pl.BlockSpec(memory_space=pltpu.VMEM),
            scratch_shapes=[
                whole, pltpu.VMEM(factors.shape, jnp.float32), whole, whole, whole, whole, whole, whole,
                dma((blocks,)), dma((levels, blocks)), dma((count,)), dma((count,)), dma((count,)),
                dma, dma, dma, dma, dma, pltpu.SemaphoreType.REGULAR, pltpu.SemaphoreType.REGULAR,
            ],
            compiler_params=pltpu.CompilerParams(
                collective_id=0, has_side_effects=True, vmem_limit_bytes=54 * 1024 * 1024
            ),
        )(coeff, factors)
        return landed

    placed = (P(("src", "tgt"), None, None), P(None, ("src", "tgt"), None, None))
    return jax.shard_map(
        local, mesh=mesh, in_specs=placed, out_specs=P("src", "tgt", None), check_vma=False
    )
```

```python
import functools

import jax
import jax.numpy as jnp
from jax import lax
from jax.experimental import pallas as pl
from jax.experimental.pallas import tpu as pltpu
from jax.sharding import PartitionSpec as P

SPLIT = 8
AHEAD = 24
FIRST = 3
LAG_B, LAG_C = 4, 6
HOLD_Y, STEP_Y = 58, 1
HOLD_XY, STEP_XY = 54, 2
ORDER = (1, 3, 2)
MESH = pl.DeviceIdType.MESH


def split(x):
    high = x.astype(jnp.bfloat16)
    return high, (x - high.astype(jnp.float32)).astype(jnp.bfloat16)


def dot(x, w):
    x_high, x_low = split(x)
    w_high, w_low = split(w)
    mm = functools.partial(jnp.dot, preferred_element_type=jnp.float32)
    return mm(x_high, w_high) + (mm(x_high, w_low) + mm(x_low, w_high))


def kernel(
    n_src, n_tgt, coeff, factors, out,
    c_v, f_v, got0, got1, got2, new0, new1, new2,
    c_sem, f_sem, got0_sem, got1_sem, got2_sem, sent0, sent1, sent2, sent3, landed, near, far,
):
    blocks, rhs, rank = c_v.shape
    rows = rhs // SPLIT
    part = rhs // n_tgt
    count = blocks * SPLIT
    src = lax.axis_index("src")
    tgt = lax.axis_index("tgt")
    half_t, half_s = n_tgt // 2, n_src // 2
    upper = (tgt // half_t, src // half_s, lax.rem(tgt, 2))
    first = (src, lax.rem(tgt + half_t, n_tgt))
    second = (lax.rem(src + half_s, n_src), tgt)
    third = (src, tgt + 1 - 2 * lax.rem(tgt, 2))

    def load_c(block):
        return pltpu.make_async_copy(coeff.at[block], c_v.at[block], c_sem.at[block])

    def load_f(level, block):
        return pltpu.make_async_copy(
            factors.at[level, block], f_v.at[level, block], f_sem.at[level, block]
        )

    def place(chunk):
        block = chunk // SPLIT
        at = pl.multiple_of(lax.rem(chunk, SPLIT) * rows, rows)
        return block, pl.ds(at, rows)

    def exchange(source, target, sent, got, device, chunk):
        block, span = place(chunk)
        return pltpu.make_async_remote_copy(
            source.at[block, span, :], target.at[block, span, :], sent, got.at[chunk],
            device_id=device, device_id_type=MESH,
        )

    def exchange0(chunk):
        return exchange(c_v, got0, sent0, got0_sem, first, chunk)

    def exchange1(chunk):
        return exchange(new0, got1, sent1, got1_sem, second, chunk)

    def exchange2(chunk):
        return exchange(new1, got2, sent2, got2_sem, third, chunk)

    def send0(chunk):
        @pl.when(lax.rem(chunk, SPLIT) == 0)
        def _():
            load_c(chunk // SPLIT).wait()

        exchange0(chunk).start()

    def combine(level, chunk, own, other, target):
        block, span = place(chunk)
        own_rows = pl.ds(pl.multiple_of(upper[level] * rank, rank), rank)
        other_rows = pl.ds(pl.multiple_of((1 - upper[level]) * rank, rank), rank)
        target[block, span, :] = dot(own[block, span, :], f_v[level, block, own_rows, :]) + dot(
            other[block, span, :], f_v[level, block, other_rows, :]
        )

    y, x, core = tgt // 4, lax.rem(tgt // 2, 2), lax.rem(tgt, 2)

    def deliver(block, dy, other_x, other_core):
        to_x = 1 - x if other_x else x
        to_core = 1 - core if other_core else core
        to = lax.rem(y + dy, n_tgt // 4) * 4 + to_x * 2 + to_core
        pltpu.make_async_remote_copy(
            new2.at[block, pl.ds(pl.multiple_of(to * part, 8), part), :],
            out.at[tgt * blocks + block], sent3, landed,
            device_id=(src, to), device_id_type=MESH,
        ).start()

    def scatter_x(block):
        out[tgt * blocks + block] = new2[block, pl.ds(pl.multiple_of(tgt * part, 8), part), :]
        for other in (0, 1):
            deliver(block, 0, 1, other)

    def scatter_y(block):
        for dy in ORDER:
            for other in (0, 1):
                deliver(block, dy, 0, other)
        deliver(block, 0, 0, 1)

    def scatter_xy(block):
        for dy in ORDER:
            for other in (0, 1):
                deliver(block, dy, 1, other)

    barrier = pltpu.get_barrier_semaphore()

    def greet(semaphore, device):
        pl.semaphore_signal(semaphore, inc=1, device_id=device, device_id_type=MESH)

    beside = (src, tgt + 2 - 4 * x)
    for dy in (2, 1, 3):
        greet(barrier, (src, lax.rem(tgt + 4 * dy, n_tgt)))
    for device in (second, beside, third):
        greet(barrier, device)
    for block in range(FIRST):
        load_c(block).start()
    load_f(0, 0).start()

    pl.semaphore_wait(barrier, 6)
    greet(near, third)

    @pl.loop(0, AHEAD)
    def _(chunk):
        send0(chunk)

    @pl.loop(1, blocks)
    def _(block):
        @pl.when(block >= FIRST)
        def _():
            load_c(block).start()

        load_f(0, block).start()

    @pl.loop(0, blocks)
    def _(block):
        load_f(1, block).start()
        load_f(2, block).start()

    pl.semaphore_wait(near, 1)
    greet(far, beside)
    pl.semaphore_wait(far, 1)

    @pl.loop(0, count + LAG_C)
    def _(step):
        @pl.when(step + AHEAD < count)
        def _():
            send0(step + AHEAD)

        @pl.when(step < count)
        def _():
            block = step // SPLIT

            @pl.when(lax.rem(step, SPLIT) == 0)
            def _():
                load_f(0, block).wait()

            exchange0(step).wait_recv()
            combine(0, step, c_v, got0, new0)
            exchange1(step).start()

        @pl.when((step >= LAG_B) & (step < count + LAG_B))
        def _():
            chunk = step - LAG_B

            @pl.when(lax.rem(chunk, SPLIT) == 0)
            def _():
                load_f(1, chunk // SPLIT).wait()

            exchange1(chunk).wait_recv()
            combine(1, chunk, new0, got1, new1)
            exchange2(chunk).start()

        @pl.when(step >= LAG_C)
        def _():
            chunk = step - LAG_C

            @pl.when(lax.rem(chunk, SPLIT) == 0)
            def _():
                load_f(2, chunk // SPLIT).wait()

            exchange2(chunk).wait_recv()
            combine(2, chunk, new1, got2, new2)

        for block in range(blocks):
            ready = (block + 1) * SPLIT - 1 + LAG_C

            @pl.when(step == max(ready, HOLD_Y + STEP_Y * min(block, blocks - 2)))
            def _(block=block):
                scatter_y(block)

            @pl.when(step == max(ready, HOLD_XY + STEP_XY * min(block, blocks - 2)))
            def _(block=block):
                scatter_xy(block)

    @pl.loop(0, blocks)
    def _(block):
        scatter_x(block)

    for copy in (
        pltpu.make_async_remote_copy(c_v, got0, sent0, landed, device_id=first, device_id_type=MESH),
        pltpu.make_async_remote_copy(new0, got1, sent1, landed, device_id=second, device_id_type=MESH),
        pltpu.make_async_remote_copy(new1, got2, sent2, landed, device_id=third, device_id_type=MESH),
    ):
        copy.wait_send()
    moved = out.at[pl.ds(0, (n_tgt - 1) * blocks)]
    last = pltpu.make_async_remote_copy(
        moved, moved, sent3, landed, device_id=third, device_id_type=MESH
    )
    last.wait_send()
    last.wait_recv()


def store(source, out, sem):
    pieces = 8
    size = source.shape[0] // pieces
    copies = [
        pltpu.make_async_copy(source.at[pl.ds(i * size, size)], out.at[pl.ds(i * size, size)], sem.at[i])
        for i in range(pieces)
    ]
    for copy in copies:
        copy.start()
    for copy in copies:
        copy.wait()


def solution(mesh):
    n_src, n_tgt = mesh.shape["src"], mesh.shape["tgt"]

    def local(coeff, factors):
        blocks, rhs, rank = coeff.shape
        levels = factors.shape[0]
        count = blocks * SPLIT
        whole = pltpu.VMEM((blocks, rhs, rank), jnp.float32)
        dma = pltpu.SemaphoreType.DMA
        shape = (n_tgt * blocks, rhs // n_tgt, rank)
        landed = pl.pallas_call(
            functools.partial(kernel, n_src, n_tgt),
            out_shape=pltpu.VMEM(shape, jnp.float32),
            in_specs=[pl.BlockSpec(memory_space=pl.ANY)] * 2,
            out_specs=pl.BlockSpec(memory_space=pltpu.VMEM),
            scratch_shapes=[
                whole, pltpu.VMEM(factors.shape, jnp.float32), whole, whole, whole, whole, whole, whole,
                dma((blocks,)), dma((levels, blocks)), dma((count,)), dma((count,)), dma((count,)),
                dma, dma, dma, dma, dma, pltpu.SemaphoreType.REGULAR, pltpu.SemaphoreType.REGULAR,
            ],
            compiler_params=pltpu.CompilerParams(
                collective_id=0, has_side_effects=True, vmem_limit_bytes=54 * 1024 * 1024
            ),
        )(coeff, factors)
        return landed

    placed = (P(("src", "tgt"), None, None), P(None, ("src", "tgt"), None, None))
    return jax.shard_map(
        local, mesh=mesh, in_specs=placed, out_specs=P("src", "tgt", None), check_vma=False
    )
```
